32 devices in a mesh: dp: 4 (over y, x), expert: 8 (over z, core).
Axes of the slice: x: 2, y: 2, z: 4, core: 2. Of those that a mesh axis runs over, the one named last changes fastest.
Arguments:
- expert_ids: int32 [1024, 4], P(('dp', 'expert')), may hold values from 0 to 7, all different within a row; in each aligned block of 32 rows (0 to 31, 32 to 63, ...) at most 20 rows name the same one
- expert_home: int32 [8], replicated, may hold values from 0 to 7, each once
- live_tokens: int32 [32], P(('dp', 'expert')), may hold values from 1 to 32, 768 in all
- gate_weights: float32 [1024, 4], P(('dp', 'expert')), may hold values from 0.1 to 1
- output_grad: bfloat16 [1024, 7168], P(('dp', 'expert')), may hold values from -6 to 6
- saved_hidden: bfloat16 [1024, 4, 1024], P(('dp', 'expert')), may hold values from -0.59765625 to 0.59765625
- down_weight: bfloat16 [8, 1024, 7168], P('expert'), may hold values from -0.1875 to 0.1875
- dense_input: bfloat16 [1024, 7168], P(('dp', 'expert')), may hold values from -6 to 6
- latent_grad: bfloat16 [1024, 256], P(('dp', 'expert')), may hold values from -0.1875 to 0.1875
Outputs:
- hidden_grad: bfloat16 [1024, 4, 1024], P(('dp', 'expert'))
- expert_grad: float32 [8, 1024, 7168], P('expert', 'dp')
- dense_grad: float32 [7168, 256], P(('dp', 'expert'))
The draws below stay inside these ranges and needn't reach their ends.
Inputs may be any that keep to these rules, and one draw needn't show every extreme that they name: `expert_ids`: each row names 4 different experts. Among the rows of one device no expert is named more than 20 times, and on some devices one expert is named exactly 20 times. A permutation: expert e is held at index expert_home[e] of the expert axis, in every dp replica. `live_tokens`: entry i is the number of real tokens at the start of device i, in the order of the joined dp and expert axes; the rest are padding. Some device has all 32 real.
All inputs are finite; a program needn't handle non-finite values.
Results may differ from the reference program's by a relative error of at most 0.008.
Values may be sent and summed in bfloat16 or wider, within the bound.
A program may use at most 192 MiB of HBM per device.

```python
import math
import jax
import jax.numpy as jnp
import numpy as np
from jax import lax

D = 7168
KVR = 256
FFE = 1024
TOK_DEV = 32
EXPERTS = 8
TOPK = 4
CAP = 20
TOKENS = 1024
N_DP = 4
DEVICES = 32


def strengthened(result, own_key, source, target, shards_of, factor):
    owner, partner = [(jnp.arange(result.shape[position]) // (result.shape[position] // shards_of)).reshape([-1 if axis == position else 1 for axis in range(result.ndim)]) for position in (source, target)]
    chosen = jax.random.permutation(own_key, shards_of)[partner]
    strong = (owner == chosen) | (owner == (partner + shards_of // 2) % shards_of)
    return jnp.where(strong, factor * result, result)


def level_of(key, shape, split, low, top_value):
    gain = 1.0
    for dim, blocks in split:
        heights = jax.random.uniform(jax.random.fold_in(jax.random.fold_in(key, 6), dim), (blocks,), jnp.float32, low / len(split), top_value / len(split))
        gain = gain * jnp.repeat(jnp.exp(heights), shape[dim] // blocks).reshape((-1,) + (1,) * (len(shape) - 1 - dim))
    return gain


def profile(count, total, bound, skew):
    loads = [(1 << 20) // math.isqrt(standing ** skew) + 1 for standing in range(2, count + 1)]
    rest, given = total - bound - (count - 1), [1] * (count - 1)
    while rest > 0:
        movable = [i for i in range(count - 1) if given[i] < bound]
        mass, left = sum([loads[i] for i in movable]), rest
        for i in movable:
            addition = min(bound - given[i], max(1, left * loads[i] // mass), rest)
            given[i] = given[i] + addition
            rest = rest - addition
    return np.array([bound] + given)


def uneven(rng, amount, total, reach, lean):
    if amount == 2:
        one = jax.random.randint(rng, (), max(1, total - reach), min(reach, total - 1) + 1)
        return jnp.stack([one, total - one])
    sizes = jnp.asarray(profile(amount, total, reach, lean), jnp.int32)
    pairs = (amount - 1) // 2
    source_of, taker = sizes[1:1 + 2 * pairs:2], sizes[2:2 + 2 * pairs:2]
    room = jnp.minimum(source_of - 1, reach - taker)
    shifted = jax.random.randint(jax.random.fold_in(rng, 1), (pairs,), 0, 1 << 20) % (room + 1)
    sizes = sizes.at[1:1 + 2 * pairs:2].set(source_of - shifted).at[2:2 + 2 * pairs:2].set(taker + shifted)
    return sizes[jax.random.permutation(jax.random.fold_in(rng, 2), amount)]


def assign_block(own_key, own, number, rows, amount, top, limit, slope):
    ranking = jax.random.permutation(own_key, amount)
    crowded, ordinary = portions_of(amount, rows * top, limit, slope, True), portions_of(amount, rows * top, limit, slope, False)
    places = jnp.arange(amount)

    def named(lengths, turn):
        used = int((lengths > 0).sum())
        fixed = max(1, used // 4)
        shifted = fixed + (places - fixed + turn * (used - fixed)) % max(1, amount - fixed)
        return jnp.zeros((amount,), jnp.int32).at[ranking[jnp.where(places < fixed, places, shifted)]].set(jnp.asarray(lengths, jnp.int32))

    lengths = jnp.where(number % 4 == 0, named(crowded, number // 4), named(ordinary, number - number // 4 - 1))
    mixed = jax.random.permutation(jax.random.fold_in(own, 3), amount)
    giver, receiver = mixed[0:amount // 2 * 2:2], mixed[1:amount // 2 * 2:2]
    margin = jnp.minimum(lengths[giver] - 1, limit - lengths[receiver]) // 2
    margin = jnp.where((giver == ranking[0]) | (receiver == ranking[0]) | (lengths[receiver] == 0), 0, jnp.maximum(margin, 0))
    shifted = jax.random.randint(jax.random.fold_in(own, 4), (amount // 2,), 0, 1 << 20) % (margin + 1)
    lengths = lengths.at[giver].add(-shifted).at[receiver].add(shifted)
    items = jnp.searchsorted(jnp.cumsum(lengths), jnp.arange(rows * top), side="right").astype(jnp.int32)
    grid = items.reshape(top, rows).T
    grid = grid[jax.random.permutation(jax.random.fold_in(own, 1), rows)]
    turn = jax.random.randint(jax.random.fold_in(own, 2), (rows, 1), 0, top)
    return jnp.take_along_axis(grid, (jnp.arange(top)[None, :] + turn) % top, axis=1)


def portions_of(count, total, reach, slope, full):
    portions = [(1 << 20) // math.isqrt(grade ** slope) + 1 for grade in range(1, count + 1)]
    largest = reach if full else min(reach, max(-(-total // count), total * portions[0] // sum(portions)))
    least = 1 if total - largest >= count - 1 else 0
    holding, spare = [largest] + [least] * (count - 1), total - largest - least * (count - 1)
    while spare > 0:
        candidates = [i for i in range(1, count) if holding[i] < largest] or [i for i in range(1, count) if holding[i] < reach]
        mass, budget = sum([portions[i] for i in candidates]), spare
        for i in candidates:
            extra = min(reach - holding[i], max(1, budget * portions[i] // mass), spare)
            holding[i] = holding[i] + extra
            spare = spare - extra
    return np.array(holding)


def centred(own_key, dims, spread, reach, split=(), kind=jnp.bfloat16):
    drawn = spread * jax.random.normal(own_key, dims, jnp.float32)
    if split:
        drawn = drawn * level_of(own_key, dims, split, -0.22, 0.18)
    return jnp.clip(drawn, -reach, reach).astype(kind)


def gaussian_with(key, extent, width, bound, split, heavy, kind=jnp.bfloat16):
    array = width * jax.random.normal(key, extent, jnp.float32)
    if split:
        array = array * level_of(key, extent, split, -0.22, 0.18)
    return jnp.clip(strengthened(array, jax.random.fold_in(key, 3), *heavy), -bound, bound).astype(kind)


def setup_inputs(seed: int = 0) -> dict:
    seeds = jax.random.split(jax.random.key(seed), 10)
    expert_ids_keys = jax.random.split(jax.random.fold_in(seeds[0], 1), TOKENS // TOK_DEV)
    expert_ids_turns = jax.random.permutation(jax.random.fold_in(seeds[0], 3), TOKENS // TOK_DEV)
    expert_ids = jax.vmap(lambda own, number: assign_block(jax.random.fold_in(seeds[0], 2), own, number, TOK_DEV, EXPERTS, TOPK, CAP, 2))(expert_ids_keys, expert_ids_turns).reshape((TOKENS, TOPK))
    expert_home = jax.random.permutation(seeds[1], EXPERTS).astype(jnp.int32)
    live_tokens = uneven(seeds[2], DEVICES, DEVICES * TOK_DEV * 3 // 4, TOK_DEV, 2).astype(jnp.int32)
    gate_weights = jnp.clip(0.1 + 0.9 * jax.random.uniform(seeds[3], (TOKENS, TOPK), jnp.float32) ** level_of(seeds[3], (TOKENS, TOPK), ((0, 32),), -0.2, 0.2), 0.1, 1.0)
    output_grad = centred(seeds[4], (TOKENS, D), 0.5, 6.0, ((0, 32),))
    saved_hidden = gaussian_with(seeds[5], (TOKENS, TOPK, FFE), 0.1, 0.59765625, ((0, 32),), (0, 2, 32, 2.75))
    down_weight = centred(seeds[6], (EXPERTS, FFE, D), FFE ** -0.5, 0.1875, ((0, 8),))
    dense_input = gaussian_with(seeds[7], (TOKENS, D), 1.0, 6.0, ((0, 32),), (0, 1, 32, 2.75))
    latent_grad = centred(seeds[8], (TOKENS, KVR), TOKENS ** -0.5, 0.1875, ((0, 32),))
    return {"expert_ids": expert_ids, "expert_home": expert_home, "live_tokens": live_tokens, "gate_weights": gate_weights, "output_grad": output_grad, "saved_hidden": saved_hidden, "down_weight": down_weight, "dense_input": dense_input, "latent_grad": latent_grad}


def reference(expert_ids, expert_home, live_tokens, gate_weights, output_grad, saved_hidden, down_weight, dense_input, latent_grad):
    token_index = jnp.arange(TOK_DEV, dtype=jnp.int32)
    is_live = (token_index[None, :] < live_tokens[:, None]).reshape(TOKENS)
    masked_grad = jnp.where(is_live[:, None], latent_grad, jnp.zeros_like(latent_grad))
    dense_grad = jnp.dot(dense_input.T, masked_grad, preferred_element_type=jnp.float32)
    pair_home = expert_home[expert_ids]
    pair_scale = gate_weights * is_live[:, None].astype(jnp.float32)
    grad_wide = output_grad.astype(jnp.float32)

    def one_expert(carry, slot):
        chosen = pair_home == slot
        coefficient = jnp.sum(jnp.where(chosen, pair_scale, jnp.float32(0.0)), axis=1)
        gated = (grad_wide * coefficient[:, None]).astype(jnp.bfloat16)
        hidden_rows = jnp.sum(jnp.where(chosen[:, :, None], saved_hidden.astype(jnp.float32), jnp.float32(0.0)), axis=1)
        expert_weight = down_weight[slot]
        input_grad = jnp.dot(gated, expert_weight.T, preferred_element_type=jnp.float32).astype(jnp.bfloat16)
        carry = jnp.where(chosen[:, :, None], input_grad[:, None, :], carry)
        replica_hidden = hidden_rows.reshape(N_DP, TOKENS // N_DP, FFE)
        replica_grad = gated.astype(jnp.float32).reshape(N_DP, TOKENS // N_DP, D)
        partial_value = jnp.einsum("rtf,rtd->rfd", replica_hidden, replica_grad)
        summed = jnp.sum(partial_value, axis=0)
        return carry, summed

    start_grad = jnp.zeros((TOKENS, TOPK, FFE), jnp.bfloat16)
    hidden_grad, expert_grad = lax.scan(one_expert, start_grad, jnp.arange(EXPERTS, dtype=jnp.int32))
    return hidden_grad, expert_grad, dense_grad
```

```python
import jax
import jax.numpy as jnp
from jax import lax
from jax.sharding import PartitionSpec as P

BOTH = ("dp", "expert")


def on_device(
    expert_ids,
    expert_home,
    live_tokens,
    gate_weights,
    output_grad,
    saved_hidden,
    down_weight,
    dense_input,
    latent_grad,
):
    n_dp = lax.axis_size("dp")
    n_group = lax.axis_size("expert")
    tok_rows, top_count = expert_ids.shape
    model_width = output_grad.shape[1]
    hidden_units = saved_hidden.shape[2]
    owned_units = hidden_units // n_dp
    is_live = jnp.arange(tok_rows, dtype=jnp.int32) < live_tokens[0]
    masked_grad = jnp.where(is_live[:, None], latent_grad, jnp.zeros_like(latent_grad))
    everyone = lax.all_gather(
        jnp.concatenate([output_grad, masked_grad], axis=1), BOTH, axis=0, tiled=True
    )
    all_grad = everyone[:, :model_width]
    all_latent = everyone[:, model_width:]
    ids_at = expert_ids[:, :, None] == jnp.arange(expert_home.shape[0], dtype=jnp.int32)
    home = jnp.sum(jnp.where(ids_at, expert_home, 0), axis=2)
    scale = jnp.where(is_live[:, None], gate_weights, 0.0)
    at_slot = home[:, :, None] == jnp.arange(n_group, dtype=jnp.int32)
    slot_scale = jnp.where(at_slot, scale[:, :, None], 0.0)
    hidden = saved_hidden.astype(jnp.float32)
    by_slot = sum(
        slot_scale[:, k].T[:, :, None] * hidden[None, :, k] for k in range(top_count)
    ).astype(jnp.bfloat16)
    by_owner = by_slot.reshape(n_group, tok_rows, n_dp, owned_units).transpose(2, 0, 1, 3)
    by_owner = by_owner.reshape(n_dp * n_group, tok_rows, owned_units)
    dense_cut = dense_input.reshape(tok_rows, n_dp * n_group, -1).transpose(1, 0, 2)
    sent = jnp.concatenate([by_owner, dense_cut], axis=2)
    got = lax.all_to_all(sent, BOTH, split_axis=0, concat_axis=0, tiled=True)
    got = got.reshape(n_dp * n_group * tok_rows, -1)
    my_hidden = got[:, :owned_units]
    my_dense = got[:, owned_units:]
    replica_rows = n_group * tok_rows
    my_replica = lax.dynamic_slice(
        everyone, (lax.axis_index("dp") * replica_rows, 0), (replica_rows, model_width)
    )
    product = lax.dot_general(
        my_replica, down_weight[0], (((1,), (1,)), ((), ())), preferred_element_type=jnp.float32
    ).astype(jnp.bfloat16)
    returned = lax.all_to_all(
        product.reshape(n_group, tok_rows, hidden_units),
        "expert",
        split_axis=0,
        concat_axis=0,
        tiled=True,
    )
    expert_grad = lax.dot_general(
        my_hidden, all_grad, (((0,), (0,)), ((), ())), preferred_element_type=jnp.float32
    )
    dense_grad = lax.dot_general(
        my_dense, all_latent, (((0,), (0,)), ((), ())), preferred_element_type=jnp.float32
    )
    returned = returned.astype(jnp.float32)
    hidden_grad = jnp.stack(
        [
            sum(slot_scale[:, k, s][:, None] * returned[s] for s in range(n_group))
            for k in range(top_count)
        ],
        axis=1,
    ).astype(jnp.bfloat16)
    return (hidden_grad, expert_grad[None], dense_grad)


def solution(mesh):
    placed = (
        P(BOTH, None),
        P(),
        P(BOTH),
        P(BOTH, None),
        P(BOTH, None),
        P(BOTH, None, None),
        P("expert", None, None),
        P(BOTH, None),
        P(BOTH, None),
    )
    return jax.shard_map(
        on_device,
        mesh=mesh,
        in_specs=placed,
        out_specs=(P(BOTH, None, None), P("expert", "dp", None), P(BOTH, None)),
        check_vma=False,
    )
```

```python
import functools
import itertools

import jax
import jax.numpy as jnp
from jax import lax
from jax.experimental import pallas as pl
from jax.experimental.pallas import tpu as pltpu
from jax.sharding import PartitionSpec as P

BOTH = ("dp", "expert")
MESH = pl.DeviceIdType.MESH


def gather_kernel(
    n_dp, n_group, chunks, x_ref, out_ref, send_sem, recv_sem, give_sem, take_sem, own_sem
):
    n_col, n_low = n_group // 2, 2
    n_high = n_dp // n_low
    swap = n_high == n_low
    dp, group = lax.axis_index("dp"), lax.axis_index("expert")
    col, core = group // 2, group % 2
    high, low = dp // n_low, dp % n_low
    sizes = (n_col, n_low, n_high)
    rows = x_ref.shape[0]
    part = rows // chunks

    def moved(step, sign):
        col_step, first, second = step
        if swap:
            low_step = first * (1 - core) + second * core
            high_step = first * core + second * (1 - core)
        else:
            low_step, high_step = first, second
        to_col = (col + sign * col_step + n_col) % n_col
        to_low = (low + sign * low_step + n_low) % n_low
        to_high = (high + sign * high_step + n_high) % n_high
        return to_high * n_low + to_low, to_col * 2 + core

    def row_span(at_dp, at_group, chunk):
        start = (at_dp * n_group + at_group) * rows + chunk * part
        return out_ref.at[pl.ds(pl.multiple_of(start, part), part)]

    def flat(step, chunk):
        return ((step[0] * sizes[1] + step[1]) * sizes[2] + step[2]) * chunks + chunk

    def children(step):
        last = max([i for i in range(3) if step[i]], default=-1)
        for dim in range(last + 1, 3):
            for hop in range(1, sizes[dim]):
                yield tuple(hop if i == dim else 0 for i in range(3))

    def source(step, chunk):
        if not any(step):
            return x_ref.at[pl.ds(chunk * part, part)]
        return row_span(*moved(step, -1), chunk)

    def forward(step, hop, chunk):
        after = tuple(a + b for a, b in zip(step, hop))
        return pltpu.make_async_remote_copy(
            src_ref=source(step, chunk),
            dst_ref=row_span(*moved(step, -1), chunk),
            send_sem=send_sem.at[flat(after, chunk)],
            recv_sem=recv_sem.at[flat(after, chunk)],
            device_id=moved(hop, 1),
            device_id_type=MESH,
        )

    def give(step, chunk):
        return pltpu.make_async_remote_copy(
            src_ref=source(step, chunk),
            dst_ref=row_span(*moved(step, -1), chunk),
            send_sem=give_sem.at[flat(step, chunk)],
            recv_sem=take_sem.at[flat(step, chunk)],
            device_id=(dp, col * 2 + 1 - core),
            device_id_type=MESH,
        )

    def arrival(span, sem):
        return pltpu.make_async_remote_copy(
            src_ref=span,
            dst_ref=span,
            send_sem=give_sem.at[0],
            recv_sem=sem,
            device_id=(dp, col * 2 + 1 - core),
            device_id_type=MESH,
        )

    start = (0, 0, 0)
    hops = list(children(start))
    barrier = pltpu.get_barrier_semaphore()
    for hop in hops:
        pl.semaphore_signal(barrier, inc=1, device_id=moved(hop, 1), device_id_type=MESH)
    pl.semaphore_signal(
        barrier, inc=1, device_id=(dp, col * 2 + 1 - core), device_id_type=MESH
    )
    pl.semaphore_wait(barrier, len(hops) + 1)

    def when(event):
        step, chunk = event
        return (1.35 * step[0] + (step[1] > 0) + 1.2 * (step[2] > 0) + 0.5 * chunk, event)

    events = sorted(
        itertools.product(itertools.product(*[range(n) for n in sizes]), range(chunks)), key=when
    )
    own = pltpu.make_async_copy(
        x_ref, out_ref.at[pl.ds((dp * n_group + group) * rows, rows)], own_sem
    )
    sent = []
    for step, chunk in events:
        if any(step):
            arrival(row_span(*moved(step, -1), chunk), recv_sem.at[flat(step, chunk)]).wait_recv()
        for hop in children(step):
            copy = forward(step, hop, chunk)
            copy.start()
            sent.append(copy)
        copy = give(step, chunk)
        copy.start()
        sent.append(copy)
    own.start()
    for step, chunk in events:
        from_dp, from_group = moved((step[0], step[2], step[1]) if swap else step, -1)
        span = row_span(from_dp, from_group + 1 - 2 * core, chunk)
        arrival(span, take_sem.at[flat(step, chunk)]).wait_recv()
    for copy in sent:
        copy.wait_send()
    own.wait()


def gather_rows(x):
    n_dp, n_group = lax.axis_size("dp"), lax.axis_size("expert")
    chunks = 2 if x.shape[0] % 32 == 0 else 1
    shards = n_dp * n_group // 2
    full = jax.ShapeDtypeStruct((n_dp * n_group * x.shape[0], x.shape[1]), x.dtype)
    sems = pltpu.SemaphoreType.DMA((shards * chunks,))
    return pl.pallas_call(
        functools.partial(gather_kernel, n_dp, n_group, chunks),
        out_shape=full,
        in_specs=[pl.BlockSpec(memory_space=pl.ANY)],
        out_specs=pl.BlockSpec(memory_space=pl.ANY),
        scratch_shapes=[sems, sems, sems, sems, pltpu.SemaphoreType.DMA],
        compiler_params=pltpu.CompilerParams(collective_id=0, has_side_effects=True),
        cost_estimate=pl.CostEstimate(
            flops=0, bytes_accessed=8 * full.size * x.dtype.itemsize, transcendentals=0
        ),
        name="gather_rows",
    )(x)


def on_device(
    expert_ids,
    expert_home,
    live_tokens,
    gate_weights,
    output_grad,
    saved_hidden,
    down_weight,
    dense_input,
    latent_grad,
):
    n_dp = lax.axis_size("dp")
    n_group = lax.axis_size("expert")
    tok_rows, top_count = expert_ids.shape
    model_width = output_grad.shape[1]
    hidden_units = saved_hidden.shape[2]
    owned_units = hidden_units // n_dp
    is_live = jnp.arange(tok_rows, dtype=jnp.int32) < live_tokens[0]
    masked_grad = jnp.where(is_live[:, None], latent_grad, jnp.zeros_like(latent_grad))
    ids_at = expert_ids[:, :, None] == jnp.arange(expert_home.shape[0], dtype=jnp.int32)
    home = jnp.sum(jnp.where(ids_at, expert_home, 0), axis=2)
    scale = jnp.where(is_live[:, None], gate_weights, 0.0)
    at_slot = home[:, :, None] == jnp.arange(n_group, dtype=jnp.int32)
    slot_scale = jnp.where(at_slot, scale[:, :, None], 0.0)
    hidden = saved_hidden.astype(jnp.float32)
    by_slot = sum(
        slot_scale[:, k].T[:, :, None] * hidden[None, :, k] for k in range(top_count)
    ).astype(jnp.bfloat16)
    by_owner = by_slot.reshape(n_group, tok_rows, n_dp, owned_units).transpose(2, 0, 1, 3)
    by_owner = by_owner.reshape(n_dp * n_group, tok_rows, owned_units)
    dense_cut = dense_input.reshape(tok_rows, n_dp * n_group, -1).transpose(1, 0, 2)
    sent = jnp.concatenate([by_owner, dense_cut], axis=2)
    sent, grads = lax.optimization_barrier(
        (sent, jnp.concatenate([output_grad, masked_grad], axis=1))
    )
    everyone = gather_rows(grads)
    all_grad = everyone[:, :model_width]
    all_latent = everyone[:, model_width:]
    got = lax.all_to_all(sent, BOTH, split_axis=0, concat_axis=0, tiled=True)
    got = got.reshape(n_dp * n_group * tok_rows, -1)
    my_hidden = got[:, :owned_units]
    my_dense = got[:, owned_units:]
    replica_rows = n_group * tok_rows
    my_replica = lax.dynamic_slice(
        everyone, (lax.axis_index("dp") * replica_rows, 0), (replica_rows, model_width)
    )
    product = lax.dot_general(
        my_replica, down_weight[0], (((1,), (1,)), ((), ())), preferred_element_type=jnp.float32
    ).astype(jnp.bfloat16)
    returned = lax.all_to_all(
        product.reshape(n_group, tok_rows, hidden_units),
        "expert",
        split_axis=0,
        concat_axis=0,
        tiled=True,
    )
    expert_grad = lax.dot_general(
        my_hidden, all_grad, (((0,), (0,)), ((), ())), preferred_element_type=jnp.float32
    )
    dense_grad = lax.dot_general(
        my_dense, all_latent, (((0,), (0,)), ((), ())), preferred_element_type=jnp.float32
    )
    returned = returned.astype(jnp.float32)
    hidden_grad = jnp.stack(
        [
            sum(slot_scale[:, k, s][:, None] * returned[s] for s in range(n_group))
            for k in range(top_count)
        ],
        axis=1,
    ).astype(jnp.bfloat16)
    return (hidden_grad, expert_grad[None], dense_grad)


def solution(mesh):
    placed = (
        P(BOTH, None),
        P(),
        P(BOTH),
        P(BOTH, None),
        P(BOTH, None),
        P(BOTH, None, None),
        P("expert", None, None),
        P(BOTH, None),
        P(BOTH, None),
    )
    return jax.shard_map(
        on_device,
        mesh=mesh,
        in_specs=placed,
        out_specs=(P(BOTH, None, None), P("expert", "dp", None), P(BOTH, None)),
        check_vma=False,
    )
```

```python
import functools
import itertools

import jax
import jax.numpy as jnp
from jax import lax
from jax.experimental import pallas as pl
from jax.experimental.pallas import tpu as pltpu
from jax.sharding import PartitionSpec as P

BOTH = ("dp", "expert")
MESH = pl.DeviceIdType.MESH


def gather_kernel(
    n_dp,
    n_group,
    chunks,
    x_ref,
    swap_ref,
    out_ref,
    got_ref,
    send_sem,
    recv_sem,
    give_sem,
    take_sem,
    post_sem,
    mail_sem,
    own_sem,
):
    n_col, n_low = n_group // 2, 2
    n_high = n_dp // n_low
    swap = n_high == n_low
    dp, group = lax.axis_index("dp"), lax.axis_index("expert")
    col, core = group // 2, group % 2
    high, low = dp // n_low, dp % n_low
    sizes = (n_col, n_low, n_high)
    rows = x_ref.shape[0]
    part = rows // chunks

    def moved(step, sign):
        col_step, first, second = step
        if swap:
            low_step = first * (1 - core) + second * core
            high_step = first * core + second * (1 - core)
        else:
            low_step, high_step = first, second
        if n_col & (n_col - 1):
            to_col = (col + sign * col_step + n_col) % n_col
        else:
            to_col = 0
            for bit in range(n_col.bit_length() - 1):
                to_col += (col // 2**bit + (col_step >> bit)) % 2 * 2**bit
        to_low = (low + sign * low_step + n_low) % n_low
        to_high = (high + sign * high_step + n_high) % n_high
        return to_high * n_low + to_low, to_col * 2 + core

    def row_span(at_dp, at_group, chunk):
        start = (at_dp * n_group + at_group) * rows + chunk * part
        return out_ref.at[pl.ds(pl.multiple_of(start, part), part)]

    def flat(step, chunk):
        return ((step[0] * sizes[1] + step[1]) * sizes[2] + step[2]) * chunks + chunk

    def children(step):
        last = max([i for i in range(3) if step[i]], default=-1)
        for dim in range(last + 1, 3):
            for hop in range(1, sizes[dim]):
                yield tuple(hop if i == dim else 0 for i in range(3))

    def source(step, chunk):
        if not any(step):
            return x_ref.at[pl.ds(chunk * part, part)]
        return row_span(*moved(step, -1), chunk)

    def forward(step, hop, chunk):
        after = tuple(a + b for a, b in zip(step, hop))
        return pltpu.make_async_remote_copy(
            src_ref=source(step, chunk),
            dst_ref=row_span(*moved(step, -1), chunk),
            send_sem=send_sem.at[flat(after, chunk)],
            recv_sem=recv_sem.at[flat(after, chunk)],
            device_id=moved(hop, 1),
            device_id_type=MESH,
        )

    def give(step, chunk):
        return pltpu.make_async_remote_copy(
            src_ref=source(step, chunk),
            dst_ref=row_span(*moved(step, -1), chunk),
            send_sem=give_sem.at[flat(step, chunk)],
            recv_sem=take_sem.at[flat(step, chunk)],
            device_id=(dp, col * 2 + 1 - core),
            device_id_type=MESH,
        )

    def arrival(span, sem):
        return pltpu.make_async_remote_copy(
            src_ref=span,
            dst_ref=span,
            send_sem=give_sem.at[0],
            recv_sem=sem,
            device_id=(dp, col * 2 + 1 - core),
            device_id_type=MESH,
        )

    me, n_all = dp * n_group + group, n_dp * n_group

    def there(hop):
        return (me + hop) % n_all

    def post(hop):
        return pltpu.make_async_remote_copy(
            src_ref=swap_ref.at[there(hop)],
            dst_ref=got_ref.at[me],
            send_sem=post_sem.at[hop],
            recv_sem=mail_sem.at[hop],
            device_id=(there(hop) // n_group, there(hop) % n_group),
            device_id_type=MESH,
        )

    barrier = pltpu.get_barrier_semaphore()

    @pl.loop(1, n_all)
    def _(hop):
        pl.semaphore_signal(
            barrier,
            inc=1,
            device_id=(there(hop) // n_group, there(hop) % n_group),
            device_id_type=MESH,
        )

    pl.semaphore_wait(barrier, n_all - 1)

    def when(event):
        step, chunk = event
        return (1.35 * step[0] + (step[1] > 0) + 1.2 * (step[2] > 0) + 0.5 * chunk, event)

    events = sorted(
        itertools.product(itertools.product(*[range(n) for n in sizes]), range(chunks)), key=when
    )
    own = pltpu.make_async_copy(x_ref, out_ref.at[pl.ds(me * rows, rows)], own_sem.at[0])
    kept = pltpu.make_async_copy(swap_ref.at[me], got_ref.at[me], own_sem.at[1])
    sent = []
    for place, (step, chunk) in enumerate(events):
        if place == chunks:

            @pl.loop(1, n_all)
            def _(hop):
                post(hop).start()

            own.start()
            kept.start()
        if any(step):
            arrival(row_span(*moved(step, -1), chunk), recv_sem.at[flat(step, chunk)]).wait_recv()
        for hop in children(step):
            copy = forward(step, hop, chunk)
            copy.start()
            sent.append(copy)
        copy = give(step, chunk)
        copy.start()
        sent.append(copy)
    for step, chunk in events:
        from_dp, from_group = moved((step[0], step[2], step[1]) if swap else step, -1)
        span = row_span(from_dp, from_group + 1 - 2 * core, chunk)
        arrival(span, take_sem.at[flat(step, chunk)]).wait_recv()
    for copy in sent:
        copy.wait_send()

    @pl.loop(1, n_all)
    def _(hop):
        post(hop).wait_send()
        arrival(got_ref.at[(me + n_all - hop) % n_all], mail_sem.at[hop]).wait_recv()

    own.wait()
    kept.wait()


def gather_and_swap(x, blocks):
    n_dp, n_group = lax.axis_size("dp"), lax.axis_size("expert")
    chunks = 2 if x.shape[0] % 32 == 0 else 1
    shards = n_dp * n_group // 2
    full = jax.ShapeDtypeStruct((n_dp * n_group * x.shape[0], x.shape[1]), x.dtype)
    sems = pltpu.SemaphoreType.DMA((shards * chunks,))
    mail_sems = pltpu.SemaphoreType.DMA((n_dp * n_group,))
    anywhere = pl.BlockSpec(memory_space=pl.ANY)
    return pl.pallas_call(
        functools.partial(gather_kernel, n_dp, n_group, chunks),
        out_shape=(full, jax.ShapeDtypeStruct(blocks.shape, blocks.dtype)),
        in_specs=[anywhere, anywhere],
        out_specs=(anywhere, anywhere),
        scratch_shapes=[
            sems,
            sems,
            sems,
            sems,
            mail_sems,
            mail_sems,
            pltpu.SemaphoreType.DMA((2,)),
        ],
        compiler_params=pltpu.CompilerParams(collective_id=0, has_side_effects=True),
        cost_estimate=pl.CostEstimate(
            flops=0, bytes_accessed=8 * full.size * x.dtype.itemsize, transcendentals=0
        ),
        name="gather_and_swap",
    )(x, blocks)


def on_device(
    expert_ids,
    expert_home,
    live_tokens,
    gate_weights,
    output_grad,
    saved_hidden,
    down_weight,
    dense_input,
    latent_grad,
):
    n_dp = lax.axis_size("dp")
    n_group = lax.axis_size("expert")
    tok_rows, top_count = expert_ids.shape
    model_width = output_grad.shape[1]
    hidden_units = saved_hidden.shape[2]
    owned_units = hidden_units // n_dp
    is_live = jnp.arange(tok_rows, dtype=jnp.int32) < live_tokens[0]
    masked_grad = jnp.where(is_live[:, None], latent_grad, jnp.zeros_like(latent_grad))
    ids_at = expert_ids[:, :, None] == jnp.arange(expert_home.shape[0], dtype=jnp.int32)
    home = jnp.sum(jnp.where(ids_at, expert_home, 0), axis=2)
    scale = jnp.where(is_live[:, None], gate_weights, 0.0)
    at_slot = home[:, :, None] == jnp.arange(n_group, dtype=jnp.int32)
    slot_scale = jnp.where(at_slot, scale[:, :, None], 0.0)
    hidden = saved_hidden.astype(jnp.float32)
    by_slot = sum(
        slot_scale[:, k].T[:, :, None] * hidden[None, :, k] for k in range(top_count)
    ).astype(jnp.bfloat16)
    by_owner = by_slot.reshape(n_group, tok_rows, n_dp, owned_units).transpose(2, 0, 1, 3)
    by_owner = by_owner.reshape(n_dp * n_group, tok_rows, owned_units)
    dense_cut = dense_input.reshape(tok_rows, n_dp * n_group, -1).transpose(1, 0, 2)
    sent = jnp.concatenate([by_owner, dense_cut], axis=2)
    grads = jnp.concatenate([output_grad, masked_grad], axis=1)
    everyone, got = gather_and_swap(grads, sent)
    all_grad = everyone[:, :model_width]
    all_latent = everyone[:, model_width:]
    got = got.reshape(n_dp * n_group * tok_rows, -1)
    my_hidden = got[:, :owned_units]
    my_dense = got[:, owned_units:]
    replica_rows = n_group * tok_rows
    my_replica = lax.dynamic_slice(
        everyone, (lax.axis_index("dp") * replica_rows, 0), (replica_rows, model_width)
    )
    product = lax.dot_general(
        my_replica, down_weight[0], (((1,), (1,)), ((), ())), preferred_element_type=jnp.float32
    ).astype(jnp.bfloat16)
    returned = lax.all_to_all(
        product.reshape(n_group, tok_rows, hidden_units),
        "expert",
        split_axis=0,
        concat_axis=0,
        tiled=True,
    )
    expert_grad = lax.dot_general(
        my_hidden, all_grad, (((0,), (0,)), ((), ())), preferred_element_type=jnp.float32
    )
    dense_grad = lax.dot_general(
        my_dense, all_latent, (((0,), (0,)), ((), ())), preferred_element_type=jnp.float32
    )
    returned = returned.astype(jnp.float32)
    hidden_grad = jnp.stack(
        [
            sum(slot_scale[:, k, s][:, None] * returned[s] for s in range(n_group))
            for k in range(top_count)
        ],
        axis=1,
    ).astype(jnp.bfloat16)
    return (hidden_grad, expert_grad[None], dense_grad)


def solution(mesh):
    placed = (
        P(BOTH, None),
        P(),
        P(BOTH),
        P(BOTH, None),
        P(BOTH, None),
        P(BOTH, None, None),
        P("expert", None, None),
        P(BOTH, None),
        P(BOTH, None),
    )
    return jax.shard_map(
        on_device,
        mesh=mesh,
        in_specs=placed,
        out_specs=(P(BOTH, None, None), P("expert", "dp", None), P(BOTH, None)),
        check_vma=False,
    )
```
